256 devices in a mesh: rows: 8 (over z), feat: 32 (over y, x, core).
Axes of the slice: x: 4, y: 4, z: 8, core: 2. Of those that a mesh axis runs over, the one named last changes fastest.
Arguments:
- codes: int32 [524288, 512], P(('rows', 'feat')), may hold values from 0 to 255, as said below
- node_ids: int32 [2, 524288], P(None, ('rows', 'feat')), may hold values from 0 to 3
- bag_counts: int32 [2, 524288], P(None, ('rows', 'feat')), may hold values from 0 to 3
- labels: int32 [524288], P(('rows', 'feat')), may hold values from 0 to 1
Outputs:
- feature_gain: float32 [2, 4, 512], P(None, None, 'feat')
- node_gain: float32 [2, 4], replicated
The draws below stay inside these ranges and needn't reach their ends.
Inputs may be any that keep to these rules, and one draw needn't show every extreme that they name: Each feature's codes lie below a cap of that feature; bins above the cap are empty.
All inputs are finite; a program needn't handle non-finite values.
Results may differ from the reference program's by a relative error of at most 0.0003.
Values sent between devices are 32-bit elements; how exact they have to be, the bound alone decides.
A program may use at most 64 MiB of HBM per device.

```python
import math
import jax
import jax.numpy as jnp
import numpy as np
from jax import lax

F = 512
BINS = 256
CLASSES = 2
TREES = 2
NODES = 4
ROWS = 524288


def draw_codes(key, part):
    first_key, second_key = jax.random.split(jax.random.fold_in(key, 11))
    raw_codes = jax.random.randint(first_key, (ROWS, F), 0, BINS, dtype=jnp.int32)
    caps = jax.random.randint(second_key, (F,), BINS // 2, BINS, dtype=jnp.int32)
    return jnp.minimum(raw_codes, caps[None, :])


def set_ends(array, key, smallest, top_value):
    longest = array.shape.index(max(array.shape))
    spots = []
    for shift in (0, 1):
        where = [jax.random.randint(jax.random.fold_in(key, axis), (), 0, length) for axis, length in enumerate(array.shape)]
        where[longest] = (where[longest] + shift) % array.shape[longest]
        spots.append(tuple(where))
    return array.at[spots[0]].set(smallest).at[spots[1]].set(top_value)


def rank_table(amount, skew):
    weights = [(1 << 20) // math.isqrt(grade ** skew) + 1 for grade in range(1, amount + 1)]
    deviation = 1 + sum(weights) // (1 << 30)
    return np.cumsum(np.array([max(1, weight // deviation) for weight in weights]))


def ranked(rng, extent, count, skew):
    grid = rank_table(count, skew)
    pick = jax.random.randint(jax.random.fold_in(rng, 1), extent, 0, int(grid[count - 1]))
    standing = jnp.searchsorted(jnp.asarray(grid, jnp.int32), pick, side="right")
    return jax.random.permutation(jax.random.fold_in(rng, 2), count)[standing].astype(jnp.int32)


def setup_inputs(seed: int = 0) -> dict:
    arg_keys = jax.random.split(jax.random.key(seed), 5)
    return {
        "codes": draw_codes(jax.random.fold_in(arg_keys[4], 71), 0),
        "node_ids": set_ends(ranked(arg_keys[1], (TREES, ROWS), NODES, 2), jax.random.fold_in(arg_keys[1], 3), 0, NODES - 1).astype(jnp.int32),
        "bag_counts": set_ends(jax.random.randint(arg_keys[2], (TREES, ROWS), 0, 4), jax.random.fold_in(arg_keys[2], 1), 0, 3).astype(jnp.int32),
        "labels": set_ends(jax.random.randint(arg_keys[3], (ROWS,), 0, CLASSES), jax.random.fold_in(arg_keys[3], 1), 0, CLASSES - 1).astype(jnp.int32),
    }


def make_weights(node_ids, bag_counts, labels):
    node_range = jnp.arange(NODES, dtype=jnp.int32)
    class_range = jnp.arange(CLASSES, dtype=jnp.int32)
    node_hit = (node_ids[:, :, None] == node_range).astype(jnp.float32)
    class_hit = (labels[:, None] == class_range).astype(jnp.float32)
    weights = bag_counts.astype(jnp.float32)[:, :, None, None] * node_hit[:, :, :, None] * class_hit[None, :, None, :]
    count_rows = labels.shape[0]
    return jnp.transpose(weights, (1, 0, 2, 3)).reshape(count_rows, TREES * NODES * CLASSES)


def split_gains(left):
    feats = left.shape[0]
    left = left.reshape(feats, TREES, NODES, CLASSES, left.shape[-1])
    total = left[..., -1:]
    n_left = jnp.sum(left, axis=3, keepdims=True)
    n_total = jnp.sum(total, axis=3, keepdims=True)
    n_right = n_total - n_left
    frac = n_left / jnp.maximum(n_total, 1.0)
    spread_terms = (left - total * frac) ** 2
    scaled = n_total / (jnp.maximum(n_left, 1.0) * jnp.maximum(n_right, 1.0))
    spread = jnp.sum(spread_terms * scaled, axis=3)
    best = jnp.max(spread, axis=-1)
    return jnp.transpose(best, (1, 2, 0))


def reference(codes, node_ids, bag_counts, labels):
    weights = make_weights(node_ids, bag_counts, labels).astype(jnp.bfloat16).astype(jnp.float32)

    def one_feature(column):
        summed = jax.ops.segment_sum(weights, column.astype(jnp.int32), num_segments=BINS)
        return jnp.transpose(summed)

    hist = lax.map(one_feature, jnp.transpose(codes))
    left = jnp.cumsum(hist, axis=2)
    feature_gain = split_gains(left)
    node_gain = jnp.max(feature_gain, axis=2)
    return feature_gain, node_gain
```

```python
import jax
import jax.numpy as jnp
from jax import lax
from jax.experimental import pallas as pl
from jax.experimental.pallas import tpu as pltpu
from jax.sharding import PartitionSpec as P

MESH = pl.DeviceIdType.MESH
BF = jnp.bfloat16
F32 = jnp.float32
I32 = jnp.int32
Z = 8
Q = 32
SIDE = 4
STEPS = 8
TILE = 256
HIGH = lax.Precision.HIGHEST


def iota(shape, axis):
    return lax.broadcasted_iota(I32, shape, axis)


def feature_of_row(row, z, core):
    other = row >> 8
    step = (row >> 5) & 7
    a = (row >> 3) & 3
    b = (row >> 1) & 3
    even = (step & 1) == 0
    x = jnp.where(even, a, b)
    y = jnp.where(even, b, a)
    owner_core = jnp.where(other == 0, core, 1 - core)
    owner_z = (step + z + 1) & 7
    return 16 * ((y * SIDE + x) * 2 + owner_core) + 2 * owner_z + (row & 1)


def sides(hi_ref, lo_ref, weights, group, k, lane, numbers):
    upper, lower = [], []
    one, zero = jnp.ones((), BF), jnp.zeros((), BF)
    for f in range(4):
        spot = (k // 8, pl.ds(group * 4 + f, 1), pl.ds(lane, TILE))
        hi = jnp.broadcast_to(hi_ref[spot], (16, TILE)).astype(BF)
        lo = jnp.broadcast_to(lo_ref[spot], (16, TILE)).astype(BF)
        for m in range(4):
            upper.append(jnp.where(hi == numbers[m], one, zero))
        for j in range(4):
            lower.append(jnp.where(lo == jnp.asarray(j, BF), weights, zero))
    return jnp.concatenate(upper, 0), jnp.concatenate(lower, 0)


def diagonal(product):
    first = iota((64, 128), 1) < 64
    return (
        jnp.where(first, product[0:64, 0:128], product[64:128, 0:128]),
        jnp.where(first, product[128:192, 128:256], product[192:256, 128:256]),
    )


def gains(hist, z):
    row, col = iota((128, 128), 0), iota((128, 128), 1)
    half = (row >> 6) == (col >> 6)
    column = (row & 15) == (col & 15)
    upto = ((row >> 4) & 3) <= ((col >> 4) & 3)
    inside = (half & column & upto).astype(F32)
    across = (half & column).astype(F32)
    before = (iota((64, 64), 1) < iota((64, 64), 0)).astype(F32)
    earlier = jnp.dot(before, hist, precision=HIGH, preferred_element_type=F32)
    left = jnp.dot(hist, inside, precision=HIGH, preferred_element_type=F32) + jnp.dot(
        earlier, across, precision=HIGH, preferred_element_type=F32
    )
    column_sum = jnp.broadcast_to(jnp.sum(hist, axis=0, keepdims=True), (8, 128))
    total = jnp.dot(column_sum, across, precision=HIGH, preferred_element_type=F32)[0:1]
    even = (iota((64, 128), 1) & 1) == 0

    def both(v):
        return v + jnp.where(even, pltpu.roll(v, 127, 1), pltpu.roll(v, 1, 1))

    total = jnp.broadcast_to(total, (64, 128))
    n_left = both(left)
    n_total = both(total)
    n_right = n_total - n_left
    frac = n_left / jnp.maximum(n_total, 1.0)
    terms = (left - total * frac) ** 2
    scaled = n_total / (jnp.maximum(n_left, 1.0) * jnp.maximum(n_right, 1.0))
    best = jnp.max(both(terms * scaled), axis=0, keepdims=True)
    best = jnp.broadcast_to(best, (8, 128))
    best = jnp.maximum(best, pltpu.roll(best, 112, 1))
    best = jnp.maximum(best, pltpu.roll(best, 96, 1))
    node, lane = iota((8, 128), 0), iota((8, 128), 1)
    picked = jnp.where((lane & 63) == 2 * node, best, 0.0)
    place = ((row >> 6) == (col & 1)) & ((col >> 1) == z)
    return jnp.dot(picked, place.astype(F32), precision=HIGH, preferred_element_type=F32)


def kernel(
    codes_ref,
    node_ref,
    bag_ref,
    label_ref,
    feature_ref,
    best_ref,
    hi_ref,
    lo_ref,
    codes_out,
    codes_in,
    weight_ref,
    weight_out,
    weight_in,
    hist,
    a1_in,
    a2_in,
    b1_in,
    b2_in,
    z_in,
    own_gain,
    gain_in,
    own_best,
    best_in,
    c_send,
    c_recv,
    ab_send,
    ab_recv,
    z_send,
    z_recv,
    g_send,
    g_recv,
    n_send,
    n_recv,
):
    z = lax.axis_index("rows")
    q = lax.axis_index("feat")
    core = lax.rem(q, 2)
    x = lax.rem(q // 2, SIDE)
    y = q // 8
    barrier = pltpu.get_barrier_semaphore()

    def greet_plane(i, carry):
        pl.semaphore_signal(
            barrier, inc=1, device_id=(z, lax.rem(q + i, Q)), device_id_type=MESH
        )
        return carry

    def greet_column(i, carry):
        pl.semaphore_signal(
            barrier, inc=1, device_id=(lax.rem(z + i, Z), q), device_id_type=MESH
        )
        return carry

    lax.fori_loop(1, Q, greet_plane, 0)
    lax.fori_loop(1, Z, greet_column, 0)

    rows = label_ref.shape[1]
    number = iota((8, rows), 0)
    parts = []
    for tree in range(2):
        key = node_ref[tree : tree + 1, :] * 2 + label_ref[...]
        bag = jnp.broadcast_to(bag_ref[tree : tree + 1, :], (8, rows))
        parts.append(jnp.where(jnp.broadcast_to(key, (8, rows)) == number, bag, 0).astype(F32))
    weight = jnp.concatenate(parts, 0)
    weight_out[...] = weight
    weight_ref[0] = weight.astype(BF)

    wanted = feature_of_row(iota((512, 512), 0), z, core)
    order = (wanted == iota((512, 512), 1)).astype(F32).astype(BF)

    def split(table):
        hi = jnp.floor(table * 0.25)
        return hi, table - 4.0 * hi

    def arrange(k, carry):
        start = pl.multiple_of(k * TILE, TILE)
        block = codes_ref[pl.ds(start, TILE), :].astype(F32).astype(BF)
        table = lax.dot_general(
            order, block, (((1,), (1,)), ((), ())), preferred_element_type=F32
        )
        hi, lo = split(table[:256])
        hi_ref[0, :, pl.ds(start, TILE)] = hi
        lo_ref[0, :, pl.ds(start, TILE)] = lo
        codes_out[:, pl.ds(start, TILE)] = table[256:]
        return carry

    lax.fori_loop(0, rows // TILE, arrange, 0)

    partner = (z, q + 1 - 2 * core)

    def code_copy(t):
        piece = pl.ds(pl.multiple_of(t * 32, 32), 32)
        return pltpu.make_async_remote_copy(
            codes_out.at[piece], codes_in.at[piece], c_send.at[t], c_recv.at[t],
            device_id=partner, device_id_type=MESH,
        )

    weight_copy = pltpu.make_async_remote_copy(
        weight_out, weight_in, c_send.at[STEPS], c_recv.at[STEPS],
        device_id=partner, device_id_type=MESH,
    )
    pl.semaphore_wait(barrier, Q - 1 + Z - 1)
    weight_copy.start()

    def send_codes(t, carry):
        code_copy(t).start()
        return carry

    lax.fori_loop(0, STEPS, send_codes, 0)
    weight_copy.wait_recv()
    weight_ref[1] = weight_in[...].astype(BF)

    def near(t, axis, way):
        on_y = lax.rem(t + axis, 2)
        on_x = 1 - on_y
        nx = lax.rem(x + on_x * way + SIDE, SIDE)
        ny = lax.rem(y + on_y * way + SIDE, SIDE)
        return (z, (ny * SIDE + nx) * 2 + core)

    def spot(t, axis, shift):
        on_y = lax.rem(t + axis, 2)
        here = on_y * y + (1 - on_y) * x
        return lax.rem(here + shift + SIDE, SIDE)

    def remote(t, kind, side, src, dst, device):
        return pltpu.make_async_remote_copy(
            src, dst, ab_send.at[t, kind, side], ab_recv.at[t, kind, side],
            device_id=device, device_id_type=MESH,
        )

    def copies_a(t, kind):
        right, left = near(t, 0, 1), near(t, 0, -1)
        if kind == 0:
            far = spot(t, 0, 2) * 4
            return (
                remote(t, 0, 0, hist.at[t, pl.ds(far, 2)], a1_in.at[t, 0], right),
                remote(t, 0, 1, hist.at[t, pl.ds(far + 2, 2)], a1_in.at[t, 1], left),
            )
        r, l = spot(t, 0, 1) * 4, spot(t, 0, -1) * 4
        first, second = (2, 0) if kind == 1 else (0, 2)
        return (
            remote(t, kind, 0, hist.at[t, pl.ds(r + first, 2)],
                   a2_in.at[t, 0, pl.ds(first, 2)], right),
            remote(t, kind, 1, hist.at[t, pl.ds(l + second, 2)],
                   a2_in.at[t, 1, pl.ds(second, 2)], left),
        )

    def copies_b(t, kind):
        right, left = near(t, 1, 1), near(t, 1, -1)
        base = spot(t, 0, 0) * 4
        top, low = pl.ds(0, 32), pl.ds(32, 32)
        if kind == 0:
            far = base + spot(t, 1, 2)
            return (
                remote(t, 3, 0, hist.at[t, far, top], b1_in.at[t, 0], right),
                remote(t, 3, 1, hist.at[t, far, low], b1_in.at[t, 1], left),
            )
        r, l = base + spot(t, 1, 1), base + spot(t, 1, -1)
        first, second = (low, top) if kind == 1 else (top, low)
        return (
            remote(t, 3 + kind, 0, hist.at[t, r, first], b2_in.at[t, 0, first], right),
            remote(t, 3 + kind, 1, hist.at[t, l, second], b2_in.at[t, 1, second], left),
        )

    def start(copies):
        for copy in copies:
            copy.start()

    def arrived(copies):
        for copy in copies:
            copy.wait_recv()

    def a1(t):
        start(copies_a(t, 0))
        start(copies_a(t, 1))

    def a2(t):
        arrived(copies_a(t, 0))
        r, l = spot(t, 0, 1) * 4, spot(t, 0, -1) * 4
        hist[t, pl.ds(r, 2)] = hist[t, pl.ds(r, 2)] + a1_in[t, 0]
        hist[t, pl.ds(l + 2, 2)] = hist[t, pl.ds(l + 2, 2)] + a1_in[t, 1]
        start(copies_a(t, 2))

    def b1(t):
        arrived(copies_a(t, 1))
        arrived(copies_a(t, 2))
        mine = pl.ds(spot(t, 0, 0) * 4, 4)
        hist[t, mine] = hist[t, mine] + (a2_in[t, 0] + a2_in[t, 1])
        start(copies_b(t, 0))
        start(copies_b(t, 1))

    def b2(t):
        arrived(copies_b(t, 0))
        base = spot(t, 0, 0) * 4
        r, l = base + spot(t, 1, 1), base + spot(t, 1, -1)
        hist[t, r, 0:32] = hist[t, r, 0:32] + b1_in[t, 0]
        hist[t, l, 32:64] = hist[t, l, 32:64] + b1_in[t, 1]
        start(copies_b(t, 2))

    def plane_sum(t):
        arrived(copies_b(t, 1))
        arrived(copies_b(t, 2))
        mine = spot(t, 0, 0) * 4 + spot(t, 1, 0)
        return mine, hist[t, mine] + (b2_in[t, 0] + b2_in[t, 1])

    def z_copy(t):
        mine = spot(t, 0, 0) * 4 + spot(t, 1, 0)
        return pltpu.make_async_remote_copy(
            hist.at[t, mine], z_in.at[t], z_send.at[t], z_recv.at[t],
            device_id=(lax.rem(z + 1 + t, Z), q), device_id_type=MESH,
        )

    def to_owner(t):
        mine, value = plane_sum(t)
        hist[t, mine] = value
        z_copy(t).start()

    count = iota((16, TILE), 0).astype(F32)
    numbers = [(count + 16.0 * m).astype(BF) for m in range(4)]

    def histogram(t, begin, end):
        def some(i, carry):
            for u in range(2):
                group = i * 2 + u
                total = None
                for k in range(16):
                    lane = (k % 8) * TILE
                    upper, lower = sides(
                        hi_ref, lo_ref, weight_ref[k // 8, :, lane : lane + TILE],
                        t * 8 + group, k, lane, numbers,
                    )
                    part = lax.dot_general(
                        upper, lower, (((1,), (1,)), ((), ())), preferred_element_type=F32
                    )
                    total = part if total is None else total + part
                hist[t, group * 2], hist[t, group * 2 + 1] = diagonal(total)
            return carry

        lax.fori_loop(begin, end, some, 0)

    def step(t, carry):
        code_copy(t).wait_recv()
        piece = pl.ds(pl.multiple_of(t * 32, 32), 32)
        hi, lo = split(codes_in[piece])
        hi_ref[1, piece] = hi
        lo_ref[1, piece] = lo
        histogram(t, 0, 2)
        pl.when(t >= 3)(lambda: to_owner(t - 3))
        pl.when(t >= 2)(lambda: b1(t - 2))
        pl.when(t >= 1)(lambda: a2(t - 1))
        histogram(t, 2, 4)
        pl.when(t >= 2)(lambda: b2(t - 2))
        a1(t)
        return carry

    lax.fori_loop(0, STEPS, step, 0)
    last = STEPS - 1
    to_owner(last - 2)
    b1(last - 1)
    a2(last)
    b2(last - 1)
    to_owner(last - 1)
    b1(last)
    b2(last)
    _, summed = plane_sum(last)
    for t in range(STEPS - 1):
        z_copy(t).wait_recv()
    summed = summed + jnp.sum(z_in[...], axis=0)

    own_gain[...] = gains(summed, z)

    def gain_copy(i):
        return pltpu.make_async_remote_copy(
            own_gain, gain_in.at[i - 1], g_send.at[i - 1], g_recv.at[i - 1],
            device_id=(lax.rem(z + i, Z), q), device_id_type=MESH,
        )

    def best_copy(i):
        return pltpu.make_async_remote_copy(
            own_best, best_in.at[i - 1], n_send.at[i - 1], n_recv.at[i - 1],
            device_id=(z, lax.rem(q + i, Q)), device_id_type=MESH,
        )

    def loop(first, end, act):
        def body(i, carry):
            act(i)
            return carry

        lax.fori_loop(first, end, body, 0)

    loop(1, Z, lambda i: gain_copy(i).start())
    loop(1, Z, lambda i: gain_copy(i).wait_recv())
    together = own_gain[...] + jnp.sum(gain_in[...], axis=0)
    feature_ref[...] = together
    own_best[...] = jnp.broadcast_to(jnp.max(together, axis=1, keepdims=True), (8, 128))
    loop(1, Q, lambda i: best_copy(i).start())

    weight_copy.wait_send()

    def leave(t):
        code_copy(t).wait_send()
        for kind in range(3):
            for copy in (*copies_a(t, kind), *copies_b(t, kind)):
                copy.wait_send()

    loop(0, STEPS, leave)
    loop(0, STEPS - 1, lambda t: z_copy(t).wait_send())
    loop(1, Z, lambda i: gain_copy(i).wait_send())
    loop(1, Q, lambda i: best_copy(i).wait_recv())
    best_ref[...] = jnp.maximum(own_best[...], jnp.max(best_in[...], axis=0))
    loop(1, Q, lambda i: best_copy(i).wait_send())


def on_device(codes, node_ids, bag_counts, labels):
    rows, features = codes.shape
    dma = pltpu.SemaphoreType.DMA
    feature_gain, node_gain = pl.pallas_call(
        kernel,
        out_shape=[jax.ShapeDtypeStruct((8, 128), F32)] * 2,
        in_specs=[pl.BlockSpec(memory_space=pltpu.VMEM)] * 4,
        out_specs=[pl.BlockSpec(memory_space=pltpu.VMEM)] * 2,
        scratch_shapes=[
            pltpu.VMEM((2, 256, rows), F32),
            pltpu.VMEM((2, 256, rows), F32),
            pltpu.VMEM((256, rows), F32),
            pltpu.VMEM((256, rows), F32),
            pltpu.VMEM((2, 16, rows), BF),
            pltpu.VMEM((16, rows), F32),
            pltpu.VMEM((16, rows), F32),
            pltpu.VMEM((STEPS, 16, 64, 128), F32),
            pltpu.VMEM((STEPS, 2, 2, 64, 128), F32),
            pltpu.VMEM((STEPS, 2, 4, 64, 128), F32),
            pltpu.VMEM((STEPS, 2, 32, 128), F32),
            pltpu.VMEM((STEPS, 2, 64, 128), F32),
            pltpu.VMEM((STEPS - 1, 64, 128), F32),
            pltpu.VMEM((8, 128), F32),
            pltpu.VMEM((Z - 1, 8, 128), F32),
            pltpu.VMEM((8, 128), F32),
            pltpu.VMEM((Q - 1, 8, 128), F32),
            dma((STEPS + 1,)),
            dma((STEPS + 1,)),
            dma((STEPS, 6, 2)),
            dma((STEPS, 6, 2)),
            dma((STEPS - 1,)),
            dma((STEPS - 1,)),
            dma((Z - 1,)),
            dma((Z - 1,)),
            dma((Q - 1,)),
            dma((Q - 1,)),
        ],
        compiler_params=pltpu.CompilerParams(
            collective_id=0, has_side_effects=True, vmem_limit_bytes=60 * 1024 * 1024
        ),
    )(codes, node_ids, bag_counts, labels.reshape(1, rows))
    return feature_gain[:, :16].reshape(2, 4, 16), node_gain[:, 0].reshape(2, 4)


def solution(mesh):
    return jax.shard_map(
        on_device,
        mesh=mesh,
        in_specs=(
            P(("rows", "feat"), None),
            P(None, ("rows", "feat")),
            P(None, ("rows", "feat")),
            P(("rows", "feat")),
        ),
        out_specs=(P(None, None, "feat"), P()),
        check_vma=False,
    )
```

```python
import jax
import jax.numpy as jnp
from jax import lax
from jax.experimental import pallas as pl
from jax.experimental.pallas import tpu as pltpu
from jax.sharding import PartitionSpec as P

MESH = pl.DeviceIdType.MESH
BF = jnp.bfloat16
F32 = jnp.float32
I32 = jnp.int32
F8 = jnp.float8_e4m3fn
Z = 8
Q = 32
SIDE = 4
STEPS = 8
TILE = 256
LOAD = 512
SCALE = 4096.0
HIGH = lax.Precision.HIGHEST


def iota(shape, axis):
    return lax.broadcasted_iota(I32, shape, axis)


def feature_of_row(row, z, core):
    other = row >> 8
    step = (row >> 5) & 7
    a = (row >> 3) & 3
    b = (row >> 1) & 3
    even = (step & 1) == 0
    x = jnp.where(even, a, b)
    y = jnp.where(even, b, a)
    owner_core = jnp.where(other == 0, core, 1 - core)
    owner_z = (step + z + 1) & 7
    return 16 * ((y * SIDE + x) * 2 + owner_core) + 2 * owner_z + (row & 1)


def sides(hi_ref, lo_ref, weights, scale, source, row, lane, numbers, quads):
    upper, lower = [], []
    zero, nothing = jnp.zeros((), BF), jnp.zeros((32, TILE), F8)
    for f in range(4):
        spot = (source, pl.ds(row + f, 1), pl.ds(lane, TILE))
        hi = jnp.broadcast_to(hi_ref[spot], (16, TILE)).astype(BF)
        lo = jnp.broadcast_to(lo_ref[spot], (32, TILE)).astype(BF)
        for m in range(2):
            upper.append(jnp.where(hi == numbers[m], scale, zero))
        for m in range(2):
            lower.append(jnp.where(lo == quads[m], weights, nothing))
    return jnp.concatenate(upper, 0), jnp.concatenate(lower, 0)


def diagonal(product):
    first = iota((32, 128), 1) < 64
    return (
        jnp.where(first, product[0:32, 0:128], product[32:64, 0:128]),
        jnp.where(first, product[64:96, 128:256], product[96:128, 128:256]),
    )


def classes(product):
    out = []
    for both in diagonal(product):
        second = jnp.floor(both * (1.0 / SCALE))
        out += [both - SCALE * second, second]
    return out


def gains(hist, z):
    row, col = iota((128, 128), 0), iota((128, 128), 1)
    half = (row >> 6) == (col >> 6)
    column = (row & 7) == (col & 7)
    upto = ((row >> 3) & 7) <= ((col >> 3) & 7)
    inside = (half & column & upto).astype(F32)
    across = (half & column).astype(F32)
    here, there = iota((64, 64), 0), iota((64, 64), 1)
    before = ((there < here) & ((there >> 5) == (here >> 5))).astype(F32)
    earlier = jnp.dot(before, hist, precision=HIGH, preferred_element_type=F32)
    left = jnp.dot(hist, inside, precision=HIGH, preferred_element_type=F32) + jnp.dot(
        earlier, across, precision=HIGH, preferred_element_type=F32
    )
    sums = jnp.concatenate(
        [
            jnp.broadcast_to(jnp.sum(hist[32 * c : 32 * c + 32], axis=0, keepdims=True), (8, 128))
            for c in range(2)
        ],
        0,
    )
    sums = jnp.dot(sums, across, precision=HIGH, preferred_element_type=F32)
    total = [jnp.broadcast_to(sums[8 * c : 8 * c + 1], (32, 128)) for c in range(2)]
    left = [left[:32], left[32:]]
    n_left = left[0] + left[1]
    n_total = total[0] + total[1]
    n_right = n_total - n_left
    frac = n_left / jnp.maximum(n_total, 1.0)
    scaled = n_total / (jnp.maximum(n_left, 1.0) * jnp.maximum(n_right, 1.0))
    spread = [(left[c] - total[c] * frac) ** 2 * scaled for c in range(2)]
    best = jnp.max(spread[0] + spread[1], axis=0, keepdims=True)
    best = jnp.broadcast_to(best, (8, 128))
    for shift in (8, 16, 32):
        best = jnp.maximum(best, pltpu.roll(best, 128 - shift, 1))
    node, lane = iota((8, 128), 0), iota((8, 128), 1)
    picked = jnp.where((lane & 63) == node, best, 0.0)
    place = ((row >> 6) == (col & 1)) & ((col >> 1) == z)
    return jnp.dot(picked, place.astype(F32), precision=HIGH, preferred_element_type=F32)


def kernel(
    codes_hbm,
    node_hbm,
    bag_hbm,
    label_hbm,
    feature_ref,
    best_ref,
    codes_ref,
    node_ref,
    bag_ref,
    label_ref,
    hi_ref,
    lo_ref,
    codes_out,
    codes_in,
    weight_ref,
    scale_ref,
    weight_out,
    weight_in,
    hist,
    a1_in,
    a2_in,
    b_in,
    z_in,
    own_gain,
    gain_in,
    own_best,
    best_in,
    load_sem,
    code_sent,
    weight_sent,
    block_sent,
    gain_sent,
    best_sent,
    code_came,
    weight_came,
    block_came,
    z_came,
    gain_came,
    best_came,
):
    rows = codes_hbm.shape[0]
    z = lax.axis_index("rows")
    q = lax.axis_index("feat")
    core = lax.rem(q, 2)
    x = lax.rem(q // 2, SIDE)
    y = q // 8
    barrier = pltpu.get_barrier_semaphore()

    def loop(first, end, act):
        def body(i, carry):
            act(i)
            return carry

        lax.fori_loop(first, end, body, 0)

    def arrived(ref, sem):
        pltpu.make_async_copy(ref, ref, sem).wait()

    pieces = rows // LOAD
    small = [
        pltpu.make_async_copy(node_hbm, node_ref, load_sem.at[pieces]),
        pltpu.make_async_copy(bag_hbm, bag_ref, load_sem.at[pieces + 1]),
        pltpu.make_async_copy(label_hbm, label_ref, load_sem.at[pieces + 2]),
    ]

    def load(k):
        piece = pl.ds(pl.multiple_of(k * LOAD, LOAD), LOAD)
        return pltpu.make_async_copy(codes_hbm.at[piece], codes_ref.at[piece], load_sem.at[k])

    def greet(z, q):
        pl.semaphore_signal(barrier, inc=1, device_id=(z, q), device_id_type=MESH)

    for copy in small:
        copy.start()
    loop(0, pieces, lambda k: load(k).start())
    loop(1, Z, lambda i: greet(lax.rem(z + i, Z), q))
    loop(1, Q, lambda i: greet(z, lax.rem(q + i, Q)))

    wanted = feature_of_row(iota((512, 512), 0), z, core)
    order = (wanted == iota((512, 512), 1)).astype(F32).astype(BF)

    for copy in small:
        copy.wait()
    number = iota((4, rows), 0)
    parts = []
    for tree in range(2):
        node = jnp.broadcast_to(node_ref[tree : tree + 1, :], (4, rows))
        bag = jnp.broadcast_to(bag_ref[tree : tree + 1, :], (4, rows))
        parts.append(jnp.where(node == number, bag, 0).astype(F32))
    weight = jnp.concatenate(parts, 0)
    scale = jnp.where(jnp.broadcast_to(label_ref[...], (8, rows)) == 1, SCALE, 1.0)
    weight_out[:8] = weight
    weight_out[8:] = scale

    def keep_weights(source, weight, scale):
        weight_ref[source] = jnp.concatenate([weight] * 4, 0).astype(BF).astype(F8)
        scale_ref[source] = jnp.concatenate([scale] * 2, 0).astype(BF)

    keep_weights(0, weight, scale)

    def split(table):
        hi = jnp.floor(table * 0.125)
        return hi, table - 8.0 * hi

    def arrange(k):
        load(k).wait()
        part = pl.ds(pl.multiple_of(k * LOAD, LOAD), LOAD)
        table = lax.dot_general(
            order, codes_ref[part, :].astype(F32).astype(BF), (((1,), (1,)), ((), ())),
            preferred_element_type=F32,
        )
        hi, lo = split(table[:256])
        hi_ref[0, :, part] = hi
        lo_ref[0, :, part] = lo
        codes_out[:, part] = table[256:]

    loop(0, pieces, arrange)

    partner = (z, q + 1 - 2 * core)

    def send_codes(t):
        piece = pl.ds(pl.multiple_of(t * 32, 32), 32)
        pltpu.make_async_remote_copy(
            codes_out.at[piece], codes_in.at[piece], code_sent, code_came.at[t],
            device_id=partner, device_id_type=MESH,
        ).start()

    pl.semaphore_wait(barrier, Q - 1 + Z - 1)
    pltpu.make_async_remote_copy(
        weight_out, weight_in, weight_sent, weight_came,
        device_id=partner, device_id_type=MESH,
    ).start()
    loop(0, STEPS, send_codes)
    arrived(weight_in, weight_came)
    keep_weights(1, weight_in[:8], weight_in[8:])

    def near(t, axis, way):
        on_y = lax.rem(t + axis, 2)
        on_x = 1 - on_y
        nx = lax.rem(x + on_x * way + SIDE, SIDE)
        ny = lax.rem(y + on_y * way + SIDE, SIDE)
        return (z, (ny * SIDE + nx) * 2 + core)

    def spot(t, axis, shift):
        on_y = lax.rem(t + axis, 2)
        here = on_y * y + (1 - on_y) * x
        return lax.rem(here + shift + SIDE, SIDE)

    def block(t, a, b=0):
        return t * 16 + a * 4 + b

    def send(t, stage, src, dst, device):
        pltpu.make_async_remote_copy(
            src, dst, block_sent, block_came.at[t, stage],
            device_id=device, device_id_type=MESH,
        ).start()

    def two(first):
        return pl.ds(first, 2)

    def a1(t):
        right, left = near(t, 0, 1), near(t, 0, -1)
        far, r, l = (block(t, spot(t, 0, shift)) for shift in (2, 1, -1))
        send(t, 0, hist.at[two(far)], a1_in.at[t, 0], right)
        send(t, 0, hist.at[two(far + 2)], a1_in.at[t, 1], left)
        send(t, 1, hist.at[two(r + 2)], a2_in.at[t, 0, two(2)], right)
        send(t, 1, hist.at[two(l)], a2_in.at[t, 1, two(0)], left)

    def a2(t):
        arrived(a1_in.at[t], block_came.at[t, 0])
        r, l = block(t, spot(t, 0, 1)), block(t, spot(t, 0, -1))
        hist[two(r)] = hist[two(r)] + a1_in[t, 0]
        hist[two(l + 2)] = hist[two(l + 2)] + a1_in[t, 1]
        send(t, 1, hist.at[two(r)], a2_in.at[t, 0, two(0)], near(t, 0, 1))
        send(t, 1, hist.at[two(l + 2)], a2_in.at[t, 1, two(2)], near(t, 0, -1))

    def b1(t):
        arrived(a2_in.at[t], block_came.at[t, 1])
        first = block(t, spot(t, 0, 0))
        mine = pl.ds(first, 4)
        hist[mine] = hist[mine] + (a2_in[t, 0] + a2_in[t, 1])
        for i, shift in enumerate((2, 1, -1)):
            send(t, 2, hist.at[first + spot(t, 1, shift)], b_in.at[t, i], near(t, 1, shift))

    def plane_sum(t):
        arrived(b_in.at[t], block_came.at[t, 2])
        mine = block(t, spot(t, 0, 0), spot(t, 1, 0))
        return mine, (hist[mine] + b_in[t, 0]) + (b_in[t, 1] + b_in[t, 2])

    def to_owner(t):
        mine, value = plane_sum(t)
        hist[mine] = value
        pltpu.make_async_remote_copy(
            hist.at[mine], z_in.at[t], block_sent, z_came,
            device_id=(lax.rem(z + 1 + t, Z), q), device_id_type=MESH,
        ).start()

    count = iota((16, TILE), 0).astype(F32)
    numbers = [(count + 16.0 * m).astype(BF) for m in range(2)]
    count = (iota((32, TILE), 0) >> 3).astype(F32)
    quads = [(count + 4.0 * m).astype(BF) for m in range(2)]
    passes = 2 * rows // TILE
    span = 1024 // TILE

    def histogram(t, begin, end):
        def some(i):
            for u in range(2):
                group = t * 8 + i * 2 + u
                counts = None
                for first in range(0, passes, span):
                    total = None
                    for k in range(first, first + span):
                        source, lane = divmod(k * TILE, rows)
                        cols = slice(lane, lane + TILE)
                        upper, lower = sides(
                            hi_ref, lo_ref, weight_ref[source, :, cols],
                            scale_ref[source, :, cols], source, group * 4, lane, numbers, quads,
                        )
                        part = lax.dot_general(
                            upper, lower, (((1,), (1,)), ((), ())), preferred_element_type=F32
                        )
                        total = part if total is None else total + part
                    more = classes(total)
                    counts = more if counts is None else [a + b for a, b in zip(counts, more)]
                for e in range(2):
                    hist[group * 2 + e, 0:32] = counts[2 * e]
                    hist[group * 2 + e, 32:64] = counts[2 * e + 1]

        loop(begin, end, some)

    def step(t):
        piece = pl.ds(pl.multiple_of(t * 32, 32), 32)
        arrived(codes_in.at[piece], code_came.at[t])
        hi, lo = split(codes_in[piece])
        hi_ref[1, piece] = hi
        lo_ref[1, piece] = lo
        histogram(t, 0, 2)
        pl.when(t >= 2)(lambda: a2(t - 2))
        pl.when(t >= 5)(lambda: to_owner(t - 5))
        histogram(t, 2, 4)
        a1(t)
        pl.when(t >= 3)(lambda: b1(t - 3))

    loop(0, STEPS, step)
    last = STEPS - 1
    a2(last - 1)
    to_owner(last - 4)
    b1(last - 2)
    a2(last)
    to_owner(last - 3)
    b1(last - 1)
    to_owner(last - 2)
    b1(last)
    to_owner(last - 1)
    _, summed = plane_sum(last)
    arrived(z_in, z_came)
    summed = summed + jnp.sum(z_in[...], axis=0)
    own_gain[...] = gains(summed, z)

    def send_gain(i):
        pltpu.make_async_remote_copy(
            own_gain, gain_in.at[i - 1], gain_sent, gain_came,
            device_id=(lax.rem(z + i, Z), q), device_id_type=MESH,
        ).start()

    def send_best(i):
        pltpu.make_async_remote_copy(
            own_best, best_in.at[i - 1], best_sent, best_came,
            device_id=(z, lax.rem(q + i, Q)), device_id_type=MESH,
        ).start()

    loop(1, Z, send_gain)
    arrived(gain_in, gain_came)
    together = own_gain[...] + jnp.sum(gain_in[...], axis=0)
    own_best[...] = jnp.broadcast_to(jnp.max(together, axis=1, keepdims=True), (8, 128))
    loop(1, Q, send_best)
    for tree in range(2):
        feature_ref[tree] = together[4 * tree : 4 * tree + 4, :16]

    arrived(weight_out, weight_sent)
    arrived(codes_out, code_sent)
    arrived(hist.at[pl.ds(0, STEPS * 16 - 1)], block_sent)
    arrived(gain_in, gain_sent)
    arrived(best_in, best_came)
    best = jnp.maximum(own_best[...], jnp.max(best_in[...], axis=0))
    for tree in range(2):
        chosen = iota((8, 128), 0) == iota((8, 128), 1) + 4 * tree
        line = jnp.sum(jnp.where(chosen, best, 0.0), axis=0, keepdims=True)
        best_ref[tree : tree + 1, :] = line[:, :4]
    arrived(best_in, best_sent)


def hand_over(feature_in, best_in, feature_ref, best_ref):
    feature_ref[...] = feature_in[...]
    best_ref[...] = best_in[...]


def on_device(codes, node_ids, bag_counts, labels):
    rows, features = codes.shape
    dma = pltpu.SemaphoreType.DMA
    whole = pl.BlockSpec(memory_space=pltpu.VMEM)
    outs = [jax.ShapeDtypeStruct((2, 4, 16), F32), jax.ShapeDtypeStruct((2, 4), F32)]
    results = pl.pallas_call(
        kernel,
        out_shape=outs,
        in_specs=[pl.BlockSpec(memory_space=pl.ANY)] * 4,
        out_specs=[whole] * 2,
        scratch_shapes=[
            pltpu.VMEM((rows, features), I32),
            pltpu.VMEM((2, rows), I32),
            pltpu.VMEM((2, rows), I32),
            pltpu.VMEM((1, rows), I32),
            pltpu.VMEM((2, 256, rows), F32),
            pltpu.VMEM((2, 256, rows), F32),
            pltpu.VMEM((256, rows), F32),
            pltpu.VMEM((256, rows), F32),
            pltpu.VMEM((2, 32, rows), F8),
            pltpu.VMEM((2, 16, rows), BF),
            pltpu.VMEM((16, rows), F32),
            pltpu.VMEM((16, rows), F32),
            pltpu.VMEM((STEPS * 16, 64, 128), F32),
            pltpu.VMEM((STEPS, 2, 2, 64, 128), F32),
            pltpu.VMEM((STEPS, 2, 4, 64, 128), F32),
            pltpu.VMEM((STEPS, 3, 64, 128), F32),
            pltpu.VMEM((STEPS - 1, 64, 128), F32),
            pltpu.VMEM((8, 128), F32),
            pltpu.VMEM((Z - 1, 8, 128), F32),
            pltpu.VMEM((8, 128), F32),
            pltpu.VMEM((Q - 1, 8, 128), F32),
            dma((rows // LOAD + 3,)),
            dma(()),
            dma(()),
            dma(()),
            dma(()),
            dma(()),
            dma((STEPS,)),
            dma(()),
            dma((STEPS, 3)),
            dma(()),
            dma(()),
            dma(()),
        ],
        compiler_params=pltpu.CompilerParams(
            collective_id=0, has_side_effects=True, vmem_limit_bytes=60 * 1024 * 1024
        ),
    )(codes, node_ids, bag_counts, labels.reshape(1, rows))
    return pl.pallas_call(
        hand_over, out_shape=outs, in_specs=[whole] * 2, out_specs=[whole] * 2
    )(*results)


def solution(mesh):
    return jax.shard_map(
        on_device,
        mesh=mesh,
        in_specs=(
            P(("rows", "feat"), None),
            P(None, ("rows", "feat")),
            P(None, ("rows", "feat")),
            P(("rows", "feat")),
        ),
        out_specs=(P(None, None, "feat"), P()),
        check_vma=False,
    )
```

```python
import jax
import jax.numpy as jnp
from jax import lax
from jax.experimental import pallas as pl
from jax.experimental.pallas import tpu as pltpu
from jax.sharding import PartitionSpec as P

MESH = pl.DeviceIdType.MESH
BF = jnp.bfloat16
F32 = jnp.float32
I32 = jnp.int32
F8 = jnp.float8_e4m3fn
Z = 8
Q = 32
SIDE = 4
STEPS = 8
TILE = 256
LOAD = 512
HALVES = 2 * STEPS
LAG_A, LAG_B, LAG_Z = 3, 6, 10
SCALE = 4096.0
HIGH = lax.Precision.HIGHEST


def iota(shape, axis):
    return lax.broadcasted_iota(I32, shape, axis)


def feature_of_row(row, z, core):
    other = row >> 8
    step = (row >> 5) & 7
    a = (row >> 3) & 3
    b = (row >> 1) & 3
    even = (step & 1) == 0
    x = jnp.where(even, a, b)
    y = jnp.where(even, b, a)
    owner_core = jnp.where(other == 0, core, 1 - core)
    owner_z = (step + z + 1) & 7
    return 16 * ((y * SIDE + x) * 2 + owner_core) + 2 * owner_z + (row & 1)


def sides(hi_ref, lo_ref, weights, scale, source, row, lane, numbers, quads):
    upper, lower = [], []
    zero, nothing = jnp.zeros((), BF), jnp.zeros((32, TILE), F8)
    for f in range(4):
        spot = (source, pl.ds(row + f, 1), pl.ds(lane, TILE))
        hi = jnp.broadcast_to(hi_ref[spot], (16, TILE)).astype(BF)
        lo = jnp.broadcast_to(lo_ref[spot], (32, TILE)).astype(BF)
        for m in range(2):
            upper.append(jnp.where(hi == numbers[m], scale, zero))
        for m in range(2):
            lower.append(jnp.where(lo == quads[m], weights, nothing))
    return jnp.concatenate(upper, 0), jnp.concatenate(lower, 0)


def diagonal(product):
    first = iota((32, 128), 1) < 64
    return (
        jnp.where(first, product[0:32, 0:128], product[32:64, 0:128]),
        jnp.where(first, product[64:96, 128:256], product[96:128, 128:256]),
    )


def classes(product):
    out = []
    for both in diagonal(product):
        second = jnp.floor(both * (1.0 / SCALE))
        out += [both - SCALE * second, second]
    return out


def gains(hist, z):
    row, col = iota((128, 128), 0), iota((128, 128), 1)
    half = (row >> 6) == (col >> 6)
    column = (row & 7) == (col & 7)
    upto = ((row >> 3) & 7) <= ((col >> 3) & 7)
    inside = (half & column & upto).astype(F32)
    across = (half & column).astype(F32)
    here, there = iota((64, 64), 0), iota((64, 64), 1)
    before = ((there < here) & ((there >> 5) == (here >> 5))).astype(F32)
    earlier = jnp.dot(before, hist, precision=HIGH, preferred_element_type=F32)
    left = jnp.dot(hist, inside, precision=HIGH, preferred_element_type=F32) + jnp.dot(
        earlier, across, precision=HIGH, preferred_element_type=F32
    )
    sums = jnp.concatenate(
        [
            jnp.broadcast_to(jnp.sum(hist[32 * c : 32 * c + 32], axis=0, keepdims=True), (8, 128))
            for c in range(2)
        ],
        0,
    )
    sums = jnp.dot(sums, across, precision=HIGH, preferred_element_type=F32)
    total = [jnp.broadcast_to(sums[8 * c : 8 * c + 1], (32, 128)) for c in range(2)]
    left = [left[:32], left[32:]]
    n_left = left[0] + left[1]
    n_total = total[0] + total[1]
    n_right = n_total - n_left
    frac = n_left / jnp.maximum(n_total, 1.0)
    scaled = n_total / (jnp.maximum(n_left, 1.0) * jnp.maximum(n_right, 1.0))
    spread = [(left[c] - total[c] * frac) ** 2 * scaled for c in range(2)]
    best = jnp.max(spread[0] + spread[1], axis=0, keepdims=True)
    best = jnp.broadcast_to(best, (8, 128))
    for shift in (8, 16, 32):
        best = jnp.maximum(best, pltpu.roll(best, 128 - shift, 1))
    node, lane = iota((8, 128), 0), iota((8, 128), 1)
    picked = jnp.where((lane & 63) == node, best, 0.0)
    place = ((row >> 6) == (col & 1)) & ((col >> 1) == z)
    return jnp.dot(picked, place.astype(F32), precision=HIGH, preferred_element_type=F32)


def kernel(
    codes_hbm,
    node_hbm,
    bag_hbm,
    label_hbm,
    feature_ref,
    best_ref,
    codes_ref,
    node_ref,
    bag_ref,
    label_ref,
    hi_ref,
    lo_ref,
    codes_out,
    codes_in,
    weight_ref,
    scale_ref,
    weight_out,
    weight_in,
    hist,
    a1_in,
    a2_in,
    b_in,
    z_in,
    own_gain,
    gain_in,
    own_best,
    best_in,
    load_sem,
    code_sent,
    weight_sent,
    block_sent,
    gain_sent,
    best_sent,
    code_came,
    weight_came,
    block_came,
    z_came,
    gain_came,
    best_came,
):
    rows = codes_hbm.shape[0]
    z = lax.axis_index("rows")
    q = lax.axis_index("feat")
    core = lax.rem(q, 2)
    x = lax.rem(q // 2, SIDE)
    y = q // 8
    barrier = pltpu.get_barrier_semaphore()

    def loop(first, end, act):
        def body(i, carry):
            act(i)
            return carry

        lax.fori_loop(first, end, body, 0)

    def arrived(ref, sem):
        pltpu.make_async_copy(ref, ref, sem).wait()

    pieces = rows // LOAD
    small = [
        pltpu.make_async_copy(node_hbm, node_ref, load_sem.at[pieces]),
        pltpu.make_async_copy(bag_hbm, bag_ref, load_sem.at[pieces + 1]),
        pltpu.make_async_copy(label_hbm, label_ref, load_sem.at[pieces + 2]),
    ]

    def load(k):
        piece = pl.ds(pl.multiple_of(k * LOAD, LOAD), LOAD)
        return pltpu.make_async_copy(codes_hbm.at[piece], codes_ref.at[piece], load_sem.at[k])

    def greet(z, q):
        pl.semaphore_signal(barrier, inc=1, device_id=(z, q), device_id_type=MESH)

    for copy in small:
        copy.start()
    loop(0, pieces, lambda k: load(k).start())
    loop(1, Z, lambda i: greet(lax.rem(z + i, Z), q))
    loop(1, Q, lambda i: greet(z, lax.rem(q + i, Q)))

    wanted = feature_of_row(iota((512, 512), 0), z, core)
    order = (wanted == iota((512, 512), 1)).astype(F32).astype(BF)

    for copy in small:
        copy.wait()
    number = iota((4, rows), 0)
    parts = []
    for tree in range(2):
        node = jnp.broadcast_to(node_ref[tree : tree + 1, :], (4, rows))
        bag = jnp.broadcast_to(bag_ref[tree : tree + 1, :], (4, rows))
        parts.append(jnp.where(node == number, bag, 0).astype(F32))
    weight = jnp.concatenate(parts, 0)
    scale = jnp.where(jnp.broadcast_to(label_ref[...], (8, rows)) == 1, SCALE, 1.0)
    weight_out[:8] = weight
    weight_out[8:] = scale

    def keep_weights(source, weight, scale):
        weight_ref[source] = jnp.concatenate([weight] * 4, 0).astype(BF).astype(F8)
        scale_ref[source] = jnp.concatenate([scale] * 2, 0).astype(BF)

    keep_weights(0, weight, scale)

    def split(table):
        hi = jnp.floor(table * 0.125)
        return hi, table - 8.0 * hi

    def arrange(k):
        load(k).wait()
        part = pl.ds(pl.multiple_of(k * LOAD, LOAD), LOAD)
        table = lax.dot_general(
            order, codes_ref[part, :].astype(F32).astype(BF), (((1,), (1,)), ((), ())),
            preferred_element_type=F32,
        )
        hi, lo = split(table[:256])
        hi_ref[0, :, part] = hi
        lo_ref[0, :, part] = lo
        codes_out[:, part] = table[256:]

    loop(0, pieces, arrange)

    partner = (z, q + 1 - 2 * core)

    def send_codes(t):
        piece = pl.ds(pl.multiple_of(t * 32, 32), 32)
        pltpu.make_async_remote_copy(
            codes_out.at[piece], codes_in.at[piece], code_sent, code_came.at[t],
            device_id=partner, device_id_type=MESH,
        ).start()

    pl.semaphore_wait(barrier, Q - 1 + Z - 1)
    pltpu.make_async_remote_copy(
        weight_out, weight_in, weight_sent, weight_came,
        device_id=partner, device_id_type=MESH,
    ).start()
    loop(0, STEPS, send_codes)
    arrived(weight_in, weight_came)
    keep_weights(1, weight_in[:8], weight_in[8:])

    def parts_of(u):
        return 2 * (u // 4) + lax.rem(u, 2), lax.rem(u // 2, 2)

    def near(t, axis, way):
        on_y = lax.rem(t + axis, 2)
        on_x = 1 - on_y
        nx = lax.rem(x + on_x * way + SIDE, SIDE)
        ny = lax.rem(y + on_y * way + SIDE, SIDE)
        return (z, (ny * SIDE + nx) * 2 + core)

    def spot(t, axis, shift):
        on_y = lax.rem(t + axis, 2)
        here = on_y * y + (1 - on_y) * x
        return lax.rem(here + shift + SIDE, SIDE)

    def block(t, a, b):
        return t * 16 + a * 4 + b

    def send(u, stage, src, dst, device):
        pltpu.make_async_remote_copy(
            src, dst, block_sent, block_came.at[u, stage],
            device_id=device, device_id_type=MESH,
        ).start()

    def a1(u):
        t, h = parts_of(u)
        right, left = near(t, 0, 1), near(t, 0, -1)
        far, r, l = (block(t, spot(t, 0, shift), 2 * h) for shift in (2, 1, -1))
        send(u, 0, hist.at[far], a1_in.at[u, 0], right)
        send(u, 0, hist.at[far + 1], a1_in.at[u, 1], left)
        send(u, 1, hist.at[r + 1], a2_in.at[u, 0, 1], right)
        send(u, 1, hist.at[l], a2_in.at[u, 1, 0], left)

    def a2(u):
        t, h = parts_of(u)
        arrived(a1_in.at[u], block_came.at[u, 0])
        r, l = (block(t, spot(t, 0, shift), 2 * h) for shift in (1, -1))
        hist[r] = hist[r] + a1_in[u, 0]
        hist[l + 1] = hist[l + 1] + a1_in[u, 1]
        send(u, 1, hist.at[r], a2_in.at[u, 0, 0], near(t, 0, 1))
        send(u, 1, hist.at[l + 1], a2_in.at[u, 1, 1], near(t, 0, -1))

    def b1(u):
        t, h = parts_of(u)
        arrived(a2_in.at[u], block_came.at[u, 1])
        first = block(t, spot(t, 0, 0), 2 * h)
        mine = pl.ds(first, 2)
        hist[mine] = hist[mine] + (a2_in[u, 0] + a2_in[u, 1])
        for e in range(2):
            away = lax.rem(2 * h + e - spot(t, 1, 0) + SIDE, SIDE)

            @pl.when(away > 0)
            def _():
                send(u, 2, hist.at[first + e], b_in.at[u, away - 1], near(t, 1, away))

    def plane_sum(u, t):
        arrived(b_in.at[u], block_came.at[u, 2])
        mine = block(t, spot(t, 0, 0), spot(t, 1, 0))
        return mine, (hist[mine] + b_in[u, 0]) + (b_in[u, 1] + b_in[u, 2])

    def to_owner(u):
        t, h = parts_of(u)

        @pl.when((spot(t, 1, 0) // 2 == h) & (t < STEPS - 1))
        def _():
            mine, value = plane_sum(u, t)
            hist[mine] = value
            pltpu.make_async_remote_copy(
                hist.at[mine], z_in.at[t], block_sent, z_came,
                device_id=(lax.rem(z + 1 + t, Z), q), device_id_type=MESH,
            ).start()

    count = iota((16, TILE), 0).astype(F32)
    numbers = [(count + 16.0 * m).astype(BF) for m in range(2)]
    count = (iota((32, TILE), 0) >> 3).astype(F32)
    quads = [(count + 4.0 * m).astype(BF) for m in range(2)]
    passes = 2 * rows // TILE
    span = 1024 // TILE

    def count_group(group):
        counts = None
        for first in range(0, passes, span):
            total = None
            for k in range(first, first + span):
                source, lane = divmod(k * TILE, rows)
                cols = slice(lane, lane + TILE)
                upper, lower = sides(
                    hi_ref, lo_ref, weight_ref[source, :, cols],
                    scale_ref[source, :, cols], source, group * 4, lane, numbers, quads,
                )
                part = lax.dot_general(
                    upper, lower, (((1,), (1,)), ((), ())), preferred_element_type=F32
                )
                total = part if total is None else total + part
            more = classes(total)
            counts = more if counts is None else [a + b for a, b in zip(counts, more)]
        for e in range(2):
            hist[group * 2 + e, 0:32] = counts[2 * e]
            hist[group * 2 + e, 32:64] = counts[2 * e + 1]

    def half_step(u):
        t, h = parts_of(u)

        @pl.when(h == 0)
        def _():
            piece = pl.ds(pl.multiple_of(t * 32, 32), 32)
            arrived(codes_in.at[piece], code_came.at[t])
            hi, lo = split(codes_in[piece])
            hi_ref[1, piece] = hi
            lo_ref[1, piece] = lo

        for a in range(SIDE):
            count_group(t * 8 + 2 * a + h)
        pl.when(u >= LAG_B)(lambda: b1(u - LAG_B))
        pl.when(u >= LAG_A)(lambda: a2(u - LAG_A))
        a1(u)
        pl.when(u >= LAG_Z)(lambda: to_owner(u - LAG_Z))

    loop(0, HALVES, half_step)

    def finish(u):
        pl.when(u < HALVES + LAG_B)(lambda: b1(u - LAG_B))
        pl.when(u < HALVES + LAG_A)(lambda: a2(u - LAG_A))
        pl.when(u < HALVES + LAG_Z)(lambda: to_owner(u - LAG_Z))

    loop(HALVES, HALVES + LAG_Z, finish)
    last = STEPS - 1
    _, summed = plane_sum(HALVES - 3 + 2 * (spot(last, 1, 0) // 2), last)
    arrived(z_in, z_came)
    summed = summed + jnp.sum(z_in[...], axis=0)
    own_gain[...] = gains(summed, z)

    def send_gain(i):
        pltpu.make_async_remote_copy(
            own_gain, gain_in.at[i - 1], gain_sent, gain_came,
            device_id=(lax.rem(z + i, Z), q), device_id_type=MESH,
        ).start()

    def send_best(i):
        pltpu.make_async_remote_copy(
            own_best, best_in.at[i - 1], best_sent, best_came,
            device_id=(z, lax.rem(q + i, Q)), device_id_type=MESH,
        ).start()

    loop(1, Z, send_gain)
    arrived(gain_in, gain_came)
    together = own_gain[...] + jnp.sum(gain_in[...], axis=0)
    own_best[...] = jnp.broadcast_to(jnp.max(together, axis=1, keepdims=True), (8, 128))
    loop(1, Q, send_best)
    for tree in range(2):
        feature_ref[tree] = together[4 * tree : 4 * tree + 4, :16]

    arrived(weight_out, weight_sent)
    arrived(codes_out, code_sent)
    arrived(hist.at[pl.ds(0, STEPS * 16 - 1)], block_sent)
    arrived(gain_in, gain_sent)
    arrived(best_in, best_came)
    best = jnp.maximum(own_best[...], jnp.max(best_in[...], axis=0))
    for tree in range(2):
        chosen = iota((8, 128), 0) == iota((8, 128), 1) + 4 * tree
        line = jnp.sum(jnp.where(chosen, best, 0.0), axis=0, keepdims=True)
        best_ref[tree : tree + 1, :] = line[:, :4]
    arrived(best_in, best_sent)


def hand_over(feature_in, best_in, feature_ref, best_ref):
    feature_ref[...] = feature_in[...]
    best_ref[...] = best_in[...]


def on_device(codes, node_ids, bag_counts, labels):
    rows, features = codes.shape
    dma = pltpu.SemaphoreType.DMA
    whole = pl.BlockSpec(memory_space=pltpu.VMEM)
    outs = [jax.ShapeDtypeStruct((2, 4, 16), F32), jax.ShapeDtypeStruct((2, 4), F32)]
    results = pl.pallas_call(
        kernel,
        out_shape=outs,
        in_specs=[pl.BlockSpec(memory_space=pl.ANY)] * 4,
        out_specs=[whole] * 2,
        scratch_shapes=[
            pltpu.VMEM((rows, features), I32),
            pltpu.VMEM((2, rows), I32),
            pltpu.VMEM((2, rows), I32),
            pltpu.VMEM((1, rows), I32),
            pltpu.VMEM((2, 256, rows), F32),
            pltpu.VMEM((2, 256, rows), F32),
            pltpu.VMEM((256, rows), F32),
            pltpu.VMEM((256, rows), F32),
            pltpu.VMEM((2, 32, rows), F8),
            pltpu.VMEM((2, 16, rows), BF),
            pltpu.VMEM((16, rows), F32),
            pltpu.VMEM((16, rows), F32),
            pltpu.VMEM((STEPS * 16, 64, 128), F32),
            pltpu.VMEM((HALVES, 2, 64, 128), F32),
            pltpu.VMEM((HALVES, 2, 2, 64, 128), F32),
            pltpu.VMEM((HALVES, 3, 64, 128), F32),
            pltpu.VMEM((STEPS - 1, 64, 128), F32),
            pltpu.VMEM((8, 128), F32),
            pltpu.VMEM((Z - 1, 8, 128), F32),
            pltpu.VMEM((8, 128), F32),
            pltpu.VMEM((Q - 1, 8, 128), F32),
            dma((rows // LOAD + 3,)),
            dma(()),
            dma(()),
            dma(()),
            dma(()),
            dma(()),
            dma((STEPS,)),
            dma(()),
            dma((HALVES, 3)),
            dma(()),
            dma(()),
            dma(()),
        ],
        compiler_params=pltpu.CompilerParams(
            collective_id=0, has_side_effects=True, vmem_limit_bytes=60 * 1024 * 1024
        ),
    )(codes, node_ids, bag_counts, labels.reshape(1, rows))
    return pl.pallas_call(
        hand_over, out_shape=outs, in_specs=[whole] * 2, out_specs=[whole] * 2
    )(*results)


def solution(mesh):
    return jax.shard_map(
        on_device,
        mesh=mesh,
        in_specs=(
            P(("rows", "feat"), None),
            P(None, ("rows", "feat")),
            P(None, ("rows", "feat")),
            P(("rows", "feat")),
        ),
        out_specs=(P(None, None, "feat"), P()),
        check_vma=False,
    )
```

```python
import jax
import jax.numpy as jnp
from jax import lax
from jax.experimental import pallas as pl
from jax.experimental.pallas import tpu as pltpu
from jax.sharding import PartitionSpec as P

MESH = pl.DeviceIdType.MESH
BF = jnp.bfloat16
F32 = jnp.float32
I32 = jnp.int32
F8 = jnp.float8_e4m3fn
Z = 8
Q = 32
SIDE = 4
STEPS = 8
TILE = 256
LOAD = 1024
HALVES = 2 * STEPS
LAG_A, LAG_B, LAG_Z = 3, 6, 10
SCALE = 4096.0
HIGH = lax.Precision.HIGHEST


def iota(shape, axis):
    return lax.broadcasted_iota(I32, shape, axis)


def feature_of_row(row, z, core):
    other = row >> 8
    step = (row >> 5) & 7
    a = (row >> 3) & 3
    b = (row >> 1) & 3
    even = (step & 1) == 0
    x = jnp.where(even, a, b)
    y = jnp.where(even, b, a)
    owner_core = jnp.where(other == 0, core, 1 - core)
    owner_z = (step + z + 1) & 7
    return 16 * ((y * SIDE + x) * 2 + owner_core) + 2 * owner_z + (row & 1)


def sides(hi_ref, lo_ref, weights, scale, source, row, lane, numbers, quads):
    upper, lower = [], []
    zero, nothing = jnp.zeros((), BF), jnp.zeros((32, TILE), F8)
    for f in range(4):
        spot = (source, pl.ds(row + f, 1), pl.ds(lane, TILE))
        hi = jnp.broadcast_to(hi_ref[spot], (16, TILE)).astype(BF)
        lo = jnp.broadcast_to(lo_ref[spot], (32, TILE)).astype(BF)
        for m in range(2):
            upper.append(jnp.where(hi == numbers[m], scale, zero))
        for m in range(2):
            lower.append(jnp.where(lo == quads[m], weights, nothing))
    return jnp.concatenate(upper, 0), jnp.concatenate(lower, 0)


def diagonal(product):
    first = iota((32, 128), 1) < 64
    return (
        jnp.where(first, product[0:32, 0:128], product[32:64, 0:128]),
        jnp.where(first, product[64:96, 128:256], product[96:128, 128:256]),
    )


def classes(product):
    out = []
    for both in diagonal(product):
        second = jnp.floor(both * (1.0 / SCALE))
        out += [both - SCALE * second, second]
    return out


def gains(hist, z):
    row, col = iota((128, 128), 0), iota((128, 128), 1)
    half = (row >> 6) == (col >> 6)
    column = (row & 7) == (col & 7)
    upto = ((row >> 3) & 7) <= ((col >> 3) & 7)
    inside = (half & column & upto).astype(F32)
    across = (half & column).astype(F32)
    here, there = iota((64, 64), 0), iota((64, 64), 1)
    before = ((there < here) & ((there >> 5) == (here >> 5))).astype(F32)
    earlier = jnp.dot(before, hist, precision=HIGH, preferred_element_type=F32)
    left = jnp.dot(hist, inside, precision=HIGH, preferred_element_type=F32) + jnp.dot(
        earlier, across, precision=HIGH, preferred_element_type=F32
    )
    sums = jnp.concatenate(
        [
            jnp.broadcast_to(jnp.sum(hist[32 * c : 32 * c + 32], axis=0, keepdims=True), (8, 128))
            for c in range(2)
        ],
        0,
    )
    sums = jnp.dot(sums, across, precision=HIGH, preferred_element_type=F32)
    total = [jnp.broadcast_to(sums[8 * c : 8 * c + 1], (32, 128)) for c in range(2)]
    left = [left[:32], left[32:]]
    n_left = left[0] + left[1]
    n_total = total[0] + total[1]
    n_right = n_total - n_left
    frac = n_left / jnp.maximum(n_total, 1.0)
    scaled = n_total / (jnp.maximum(n_left, 1.0) * jnp.maximum(n_right, 1.0))
    spread = [(left[c] - total[c] * frac) ** 2 * scaled for c in range(2)]
    best = jnp.max(spread[0] + spread[1], axis=0, keepdims=True)
    best = jnp.broadcast_to(best, (8, 128))
    for shift in (8, 16, 32):
        best = jnp.maximum(best, pltpu.roll(best, 128 - shift, 1))
    node, lane = iota((8, 128), 0), iota((8, 128), 1)
    picked = jnp.where((lane & 63) == node, best, 0.0)
    place = ((row >> 6) == (col & 1)) & ((col >> 1) == z)
    return jnp.dot(picked, place.astype(F32), precision=HIGH, preferred_element_type=F32)


def kernel(
    codes_hbm,
    node_hbm,
    bag_hbm,
    label_hbm,
    feature_ref,
    best_ref,
    codes_ref,
    node_ref,
    bag_ref,
    label_ref,
    hi_ref,
    lo_ref,
    codes_out,
    codes_in,
    weight_ref,
    scale_ref,
    weight_out,
    weight_in,
    hist,
    a1_in,
    a2_in,
    b_in,
    z_in,
    own_gain,
    gain_in,
    own_best,
    best_in,
    load_sem,
    code_sent,
    weight_sent,
    block_sent,
    gain_sent,
    best_sent,
    code_came,
    weight_came,
    block_came,
    z_came,
    gain_came,
    best_came,
):
    rows = codes_hbm.shape[0]
    z = lax.axis_index("rows")
    q = lax.axis_index("feat")
    core = lax.rem(q, 2)
    x = lax.rem(q // 2, SIDE)
    y = q // 8
    barrier = pltpu.get_barrier_semaphore()

    def loop(first, end, act):
        def body(i, carry):
            act(i)
            return carry

        lax.fori_loop(first, end, body, 0)

    def arrived(ref, sem):
        pltpu.make_async_copy(ref, ref, sem).wait()

    pieces = rows // LOAD
    small = [
        pltpu.make_async_copy(node_hbm, node_ref, load_sem.at[pieces]),
        pltpu.make_async_copy(bag_hbm, bag_ref, load_sem.at[pieces + 1]),
        pltpu.make_async_copy(label_hbm, label_ref, load_sem.at[pieces + 2]),
    ]

    def load(k):
        piece = pl.ds(pl.multiple_of(k * LOAD, LOAD), LOAD)
        return pltpu.make_async_copy(codes_hbm.at[piece], codes_ref.at[piece], load_sem.at[k])

    def greet(z, q):
        pl.semaphore_signal(barrier, inc=1, device_id=(z, q), device_id_type=MESH)

    for copy in small:
        copy.start()
    loop(0, pieces, lambda k: load(k).start())
    loop(1, Z, lambda i: greet(lax.rem(z + i, Z), q))
    loop(1, Q, lambda i: greet(z, lax.rem(q + i, Q)))

    wanted = feature_of_row(iota((512, 512), 0), z, core)
    order = (wanted == iota((512, 512), 1)).astype(F32).astype(BF)

    for copy in small:
        copy.wait()
    number = iota((4, rows), 0)
    parts = []
    for tree in range(2):
        node = jnp.broadcast_to(node_ref[tree : tree + 1, :], (4, rows))
        bag = jnp.broadcast_to(bag_ref[tree : tree + 1, :], (4, rows))
        parts.append(jnp.where(node == number, bag, 0).astype(F32))
    weight = jnp.concatenate(parts, 0)
    scale = jnp.where(jnp.broadcast_to(label_ref[...], (8, rows)) == 1, SCALE, 1.0)
    weight_out[:8] = weight
    weight_out[8:] = scale

    def keep_weights(source, weight, scale):
        weight_ref[source] = jnp.concatenate([weight] * 4, 0).astype(BF).astype(F8)
        scale_ref[source] = jnp.concatenate([scale] * 2, 0).astype(BF)

    keep_weights(0, weight, scale)

    def split(table):
        hi = jnp.floor(table * 0.125)
        return hi, table - 8.0 * hi

    def arrange(k):
        load(k).wait()
        part = pl.ds(pl.multiple_of(k * LOAD, LOAD), LOAD)
        table = lax.dot_general(
            order, codes_ref[part, :].astype(F32).astype(BF), (((1,), (1,)), ((), ())),
            preferred_element_type=F32,
        )
        hi, lo = split(table[:256])
        hi_ref[0, :, part] = hi
        lo_ref[0, :, part] = lo
        codes_out[:, part] = table[256:]

    loop(0, pieces, arrange)

    partner = (z, q + 1 - 2 * core)

    def send_codes(t):
        piece = pl.ds(pl.multiple_of(t * 32, 32), 32)
        pltpu.make_async_remote_copy(
            codes_out.at[piece], codes_in.at[piece], code_sent, code_came.at[t],
            device_id=partner, device_id_type=MESH,
        ).start()

    pl.semaphore_wait(barrier, Q - 1 + Z - 1)
    pltpu.make_async_remote_copy(
        weight_out, weight_in, weight_sent, weight_came,
        device_id=partner, device_id_type=MESH,
    ).start()
    loop(0, STEPS, send_codes)
    arrived(weight_in, weight_came)
    keep_weights(1, weight_in[:8], weight_in[8:])

    def parts_of(u):
        ends = u >= HALVES - 4
        t = jnp.where(ends, u // 2, 2 * (u // 4) + lax.rem(u, 2))
        return t, jnp.where(ends, lax.rem(u, 2), lax.rem(u // 2, 2))

    def near(t, axis, way):
        on_y = lax.rem(t + axis, 2)
        on_x = 1 - on_y
        nx = lax.rem(x + on_x * way + SIDE, SIDE)
        ny = lax.rem(y + on_y * way + SIDE, SIDE)
        return (z, (ny * SIDE + nx) * 2 + core)

    def spot(t, axis, shift):
        on_y = lax.rem(t + axis, 2)
        here = on_y * y + (1 - on_y) * x
        return lax.rem(here + shift + SIDE, SIDE)

    def block(t, a, b):
        return t * 16 + a * 4 + b

    def send(u, stage, src, dst, device):
        pltpu.make_async_remote_copy(
            src, dst, block_sent, block_came.at[u, stage],
            device_id=device, device_id_type=MESH,
        ).start()

    def a1(u):
        t, h = parts_of(u)
        right, left = near(t, 0, 1), near(t, 0, -1)
        far, r, l = (block(t, spot(t, 0, shift), 2 * h) for shift in (2, 1, -1))
        send(u, 0, hist.at[far], a1_in.at[u, 0], right)
        send(u, 0, hist.at[far + 1], a1_in.at[u, 1], left)
        send(u, 1, hist.at[r + 1], a2_in.at[u, 0, 1], right)
        send(u, 1, hist.at[l], a2_in.at[u, 1, 0], left)

    def a2(u):
        t, h = parts_of(u)
        arrived(a1_in.at[u], block_came.at[u, 0])
        r, l = (block(t, spot(t, 0, shift), 2 * h) for shift in (1, -1))
        hist[r] = hist[r] + a1_in[u, 0]
        hist[l + 1] = hist[l + 1] + a1_in[u, 1]
        send(u, 1, hist.at[r], a2_in.at[u, 0, 0], near(t, 0, 1))
        send(u, 1, hist.at[l + 1], a2_in.at[u, 1, 1], near(t, 0, -1))

    def b1(u):
        t, h = parts_of(u)
        arrived(a2_in.at[u], block_came.at[u, 1])
        first = block(t, spot(t, 0, 0), 2 * h)
        mine = pl.ds(first, 2)
        hist[mine] = hist[mine] + (a2_in[u, 0] + a2_in[u, 1])
        for e in range(2):
            away = lax.rem(2 * h + e - spot(t, 1, 0) + SIDE, SIDE)

            @pl.when(away > 0)
            def _():
                send(u, 2, hist.at[first + e], b_in.at[u, away - 1], near(t, 1, away))

    def plane_sum(u, t):
        arrived(b_in.at[u], block_came.at[u, 2])
        mine = block(t, spot(t, 0, 0), spot(t, 1, 0))
        return mine, (hist[mine] + b_in[u, 0]) + (b_in[u, 1] + b_in[u, 2])

    def to_owner(u):
        t, h = parts_of(u)

        @pl.when((spot(t, 1, 0) // 2 == h) & (t < STEPS - 1))
        def _():
            mine, value = plane_sum(u, t)
            hist[mine] = value
            pltpu.make_async_remote_copy(
                hist.at[mine], z_in.at[t], block_sent, z_came,
                device_id=(lax.rem(z + 1 + t, Z), q), device_id_type=MESH,
            ).start()

    count = iota((16, TILE), 0).astype(F32)
    numbers = [(count + 16.0 * m).astype(BF) for m in range(2)]
    count = (iota((32, TILE), 0) >> 3).astype(F32)
    quads = [(count + 4.0 * m).astype(BF) for m in range(2)]
    passes = 2 * rows // TILE
    span = 1024 // TILE

    def count_group(group):
        counts = None
        for first in range(0, passes, span):
            total = None
            for k in range(first, first + span):
                source, lane = divmod(k * TILE, rows)
                cols = slice(lane, lane + TILE)
                upper, lower = sides(
                    hi_ref, lo_ref, weight_ref[source, :, cols],
                    scale_ref[source, :, cols], source, group * 4, lane, numbers, quads,
                )
                part = lax.dot_general(
                    upper, lower, (((1,), (1,)), ((), ())), preferred_element_type=F32
                )
                total = part if total is None else total + part
            more = classes(total)
            counts = more if counts is None else [a + b for a, b in zip(counts, more)]
        for e in range(2):
            hist[group * 2 + e, 0:32] = counts[2 * e]
            hist[group * 2 + e, 32:64] = counts[2 * e + 1]

    def half_step(u):
        t, h = parts_of(u)

        @pl.when(h == 0)
        def _():
            piece = pl.ds(pl.multiple_of(t * 32, 32), 32)
            arrived(codes_in.at[piece], code_came.at[t])
            hi, lo = split(codes_in[piece])
            hi_ref[1, piece] = hi
            lo_ref[1, piece] = lo

        for a in range(SIDE):
            count_group(t * 8 + 2 * a + h)
        pl.when(u >= LAG_B)(lambda: b1(u - LAG_B))
        pl.when(u >= LAG_A)(lambda: a2(u - LAG_A))
        a1(u)
        pl.when(u >= LAG_Z)(lambda: to_owner(u - LAG_Z))

    loop(0, HALVES, half_step)

    def finish(u):
        pl.when(u < HALVES + LAG_A)(lambda: a2(u - LAG_A))
        pl.when(u < HALVES + LAG_B)(lambda: b1(u - LAG_B))
        pl.when(u < HALVES + LAG_Z)(lambda: to_owner(u - LAG_Z))

    loop(HALVES, HALVES + LAG_Z, finish)
    last = STEPS - 1
    _, summed = plane_sum(HALVES - 2 + spot(last, 1, 0) // 2, last)
    arrived(z_in, z_came)
    summed = summed + jnp.sum(z_in[...], axis=0)
    own_gain[...] = gains(summed, z)

    def send_gain(i):
        pltpu.make_async_remote_copy(
            own_gain, gain_in.at[i - 1], gain_sent, gain_came,
            device_id=(lax.rem(z + i, Z), q), device_id_type=MESH,
        ).start()

    def send_best(i):
        pltpu.make_async_remote_copy(
            own_best, best_in.at[i - 1], best_sent, best_came,
            device_id=(z, lax.rem(q + i, Q)), device_id_type=MESH,
        ).start()

    loop(1, Z, send_gain)
    arrived(gain_in, gain_came)
    together = own_gain[...] + jnp.sum(gain_in[...], axis=0)
    own_best[...] = jnp.broadcast_to(jnp.max(together, axis=1, keepdims=True), (8, 128))
    loop(0, Q - 1, lambda i: send_best(lax.rem(i + 18, Q - 1) + 1))
    for tree in range(2):
        feature_ref[tree] = together[4 * tree : 4 * tree + 4, :16]

    arrived(weight_out, weight_sent)
    arrived(codes_out, code_sent)
    arrived(hist.at[pl.ds(0, STEPS * 16 - 1)], block_sent)
    arrived(gain_in, gain_sent)
    arrived(best_in, best_came)
    best = jnp.maximum(own_best[...], jnp.max(best_in[...], axis=0))
    for tree in range(2):
        chosen = iota((8, 128), 0) == iota((8, 128), 1) + 4 * tree
        line = jnp.sum(jnp.where(chosen, best, 0.0), axis=0, keepdims=True)
        best_ref[tree : tree + 1, :] = line[:, :4]
    arrived(best_in, best_sent)


def hand_over(feature_in, best_in, feature_ref, best_ref):
    feature_ref[...] = feature_in[...]
    best_ref[...] = best_in[...]


def on_device(codes, node_ids, bag_counts, labels):
    rows, features = codes.shape
    dma = pltpu.SemaphoreType.DMA
    whole = pl.BlockSpec(memory_space=pltpu.VMEM)
    outs = [jax.ShapeDtypeStruct((2, 4, 16), F32), jax.ShapeDtypeStruct((2, 4), F32)]
    results = pl.pallas_call(
        kernel,
        out_shape=outs,
        in_specs=[pl.BlockSpec(memory_space=pl.ANY)] * 4,
        out_specs=[whole] * 2,
        scratch_shapes=[
            pltpu.VMEM((rows, features), I32),
            pltpu.VMEM((2, rows), I32),
            pltpu.VMEM((2, rows), I32),
            pltpu.VMEM((1, rows), I32),
            pltpu.VMEM((2, 256, rows), F32),
            pltpu.VMEM((2, 256, rows), F32),
            pltpu.VMEM((256, rows), F32),
            pltpu.VMEM((256, rows), F32),
            pltpu.VMEM((2, 32, rows), F8),
            pltpu.VMEM((2, 16, rows), BF),
            pltpu.VMEM((16, rows), F32),
            pltpu.VMEM((16, rows), F32),
            pltpu.VMEM((STEPS * 16, 64, 128), F32),
            pltpu.VMEM((HALVES, 2, 64, 128), F32),
            pltpu.VMEM((HALVES, 2, 2, 64, 128), F32),
            pltpu.VMEM((HALVES, 3, 64, 128), F32),
            pltpu.VMEM((STEPS - 1, 64, 128), F32),
            pltpu.VMEM((8, 128), F32),
            pltpu.VMEM((Z - 1, 8, 128), F32),
            pltpu.VMEM((8, 128), F32),
            pltpu.VMEM((Q - 1, 8, 128), F32),
            dma((rows // LOAD + 3,)),
            dma(()),
            dma(()),
            dma(()),
            dma(()),
            dma(()),
            dma((STEPS,)),
            dma(()),
            dma((HALVES, 3)),
            dma(()),
            dma(()),
            dma(()),
        ],
        compiler_params=pltpu.CompilerParams(
            collective_id=0, has_side_effects=True, vmem_limit_bytes=60 * 1024 * 1024
        ),
    )(codes, node_ids, bag_counts, labels.reshape(1, rows))
    return pl.pallas_call(
        hand_over, out_shape=outs, in_specs=[whole] * 2, out_specs=[whole] * 2
    )(*results)


def solution(mesh):
    return jax.shard_map(
        on_device,
        mesh=mesh,
        in_specs=(
            P(("rows", "feat"), None),
            P(None, ("rows", "feat")),
            P(None, ("rows", "feat")),
            P(("rows", "feat")),
        ),
        out_specs=(P(None, None, "feat"), P()),
        check_vma=False,
    )
```

```python
import jax
import jax.numpy as jnp
from jax import lax
from jax.experimental import pallas as pl
from jax.experimental.pallas import tpu as pltpu
from jax.sharding import PartitionSpec as P

MESH = pl.DeviceIdType.MESH
BF = jnp.bfloat16
F32 = jnp.float32
I32 = jnp.int32
F8 = jnp.float8_e4m3fn
Z = 8
Q = 32
SIDE = 4
STEPS = 8
TILE = 256
LOAD = 1024
HALVES = 2 * STEPS
LAG_A, LAG_B, LAG_Z = 3, 6, 10
SCALE = 4096.0
HIGH = lax.Precision.HIGHEST


def iota(shape, axis):
    return lax.broadcasted_iota(I32, shape, axis)


def feature_of_row(row, z, core):
    other = row >> 8
    step = (row >> 5) & 7
    a = (row >> 3) & 3
    b = (row >> 1) & 3
    even = (step & 1) == 0
    x = jnp.where(even, a, b)
    y = jnp.where(even, b, a)
    owner_core = jnp.where(other == 0, core, 1 - core)
    owner_z = (step + z + 1) & 7
    return 16 * ((y * SIDE + x) * 2 + owner_core) + 2 * owner_z + (row & 1)


def sides(hi_ref, lo_ref, weights, scale, source, row, lane, numbers, quads):
    upper, lower = [], []
    zero, nothing = jnp.zeros((), BF), jnp.zeros((32, TILE), F8)
    for f in range(4):
        spot = (source, pl.ds(row + f, 1), pl.ds(lane, TILE))
        hi = jnp.broadcast_to(hi_ref[spot], (16, TILE)).astype(BF)
        lo = jnp.broadcast_to(lo_ref[spot], (32, TILE)).astype(BF)
        for m in range(2):
            upper.append(jnp.where(hi == numbers[m], scale, zero))
        for m in range(2):
            lower.append(jnp.where(lo == quads[m], weights, nothing))
    return jnp.concatenate(upper, 0), jnp.concatenate(lower, 0)


def diagonal(product):
    first = iota((32, 128), 1) < 64
    return (
        jnp.where(first, product[0:32, 0:128], product[32:64, 0:128]),
        jnp.where(first, product[64:96, 128:256], product[96:128, 128:256]),
    )


def classes(product):
    out = []
    for both in diagonal(product):
        second = jnp.floor(both * (1.0 / SCALE))
        out += [both - SCALE * second, second]
    return out


def gains(hist, z):
    row, col = iota((128, 128), 0), iota((128, 128), 1)
    half = (row >> 6) == (col >> 6)
    column = (row & 7) == (col & 7)
    upto = ((row >> 3) & 7) <= ((col >> 3) & 7)
    inside = (half & column & upto).astype(F32)
    across = (half & column).astype(F32)
    here, there = iota((64, 64), 0), iota((64, 64), 1)
    before = ((there < here) & ((there >> 5) == (here >> 5))).astype(F32)
    earlier = jnp.dot(before, hist, precision=HIGH, preferred_element_type=F32)
    left = jnp.dot(hist, inside, precision=HIGH, preferred_element_type=F32) + jnp.dot(
        earlier, across, precision=HIGH, preferred_element_type=F32
    )
    sums = jnp.concatenate(
        [
            jnp.broadcast_to(jnp.sum(hist[32 * c : 32 * c + 32], axis=0, keepdims=True), (8, 128))
            for c in range(2)
        ],
        0,
    )
    sums = jnp.dot(sums, across, precision=HIGH, preferred_element_type=F32)
    total = [jnp.broadcast_to(sums[8 * c : 8 * c + 1], (32, 128)) for c in range(2)]
    left = [left[:32], left[32:]]
    n_left = left[0] + left[1]
    n_total = total[0] + total[1]
    n_right = n_total - n_left
    frac = n_left / jnp.maximum(n_total, 1.0)
    scaled = n_total / (jnp.maximum(n_left, 1.0) * jnp.maximum(n_right, 1.0))
    spread = [(left[c] - total[c] * frac) ** 2 * scaled for c in range(2)]
    best = jnp.max(spread[0] + spread[1], axis=0, keepdims=True)
    best = jnp.broadcast_to(best, (8, 128))
    for shift in (8, 16, 32):
        best = jnp.maximum(best, pltpu.roll(best, 128 - shift, 1))
    node, lane = iota((8, 128), 0), iota((8, 128), 1)
    picked = jnp.where((lane & 63) == node, best, 0.0)
    place = ((row >> 6) == (col & 1)) & ((col >> 1) == z)
    return jnp.dot(picked, place.astype(F32), precision=HIGH, preferred_element_type=F32)


def kernel(
    codes_hbm,
    node_hbm,
    bag_hbm,
    label_hbm,
    feature_ref,
    best_ref,
    codes_ref,
    node_ref,
    bag_ref,
    label_ref,
    hi_ref,
    lo_ref,
    codes_out,
    codes_in,
    weight_ref,
    scale_ref,
    weight_out,
    weight_in,
    hist,
    a1_in,
    a2_in,
    b_in,
    z_in,
    own_gain,
    gain_in,
    own_best,
    best_in,
    load_sem,
    code_sent,
    weight_sent,
    block_sent,
    gain_sent,
    best_sent,
    code_came,
    weight_came,
    block_came,
    z_came,
    gain_came,
    best_came,
):
    rows = codes_hbm.shape[0]
    z = lax.axis_index("rows")
    q = lax.axis_index("feat")
    core = lax.rem(q, 2)
    x = lax.rem(q // 2, SIDE)
    y = q // 8
    barrier = pltpu.get_barrier_semaphore()

    def loop(first, end, act):
        def body(i, carry):
            act(i)
            return carry

        lax.fori_loop(first, end, body, 0)

    def arrived(ref, sem):
        pltpu.make_async_copy(ref, ref, sem).wait()

    pieces = rows // LOAD
    small = [
        pltpu.make_async_copy(node_hbm, node_ref, load_sem.at[pieces]),
        pltpu.make_async_copy(bag_hbm, bag_ref, load_sem.at[pieces + 1]),
        pltpu.make_async_copy(label_hbm, label_ref, load_sem.at[pieces + 2]),
    ]

    def load(k):
        piece = pl.ds(pl.multiple_of(k * LOAD, LOAD), LOAD)
        return pltpu.make_async_copy(codes_hbm.at[piece], codes_ref.at[piece], load_sem.at[k])

    def greet(z, q):
        pl.semaphore_signal(barrier, inc=1, device_id=(z, q), device_id_type=MESH)

    for copy in small:
        copy.start()
    loop(0, pieces, lambda k: load(k).start())
    loop(1, Z, lambda i: greet(lax.rem(z + i, Z), q))
    loop(1, Q, lambda i: greet(z, lax.rem(q + i, Q)))

    wanted = feature_of_row(iota((512, 512), 0), z, core)
    order = (wanted == iota((512, 512), 1)).astype(F32).astype(BF)

    for copy in small:
        copy.wait()
    number = iota((4, rows), 0)
    parts = []
    for tree in range(2):
        node = jnp.broadcast_to(node_ref[tree : tree + 1, :], (4, rows))
        bag = jnp.broadcast_to(bag_ref[tree : tree + 1, :], (4, rows))
        parts.append(jnp.where(node == number, bag, 0).astype(F32))
    weight = jnp.concatenate(parts, 0)
    scale = jnp.where(jnp.broadcast_to(label_ref[...], (8, rows)) == 1, SCALE, 1.0)
    weight_out[:8] = weight
    weight_out[8:] = scale

    def keep_weights(source, weight, scale):
        weight_ref[source] = jnp.concatenate([weight] * 4, 0).astype(BF).astype(F8)
        scale_ref[source] = jnp.concatenate([scale] * 2, 0).astype(BF)

    keep_weights(0, weight, scale)

    def split(table):
        hi = jnp.floor(table * 0.125)
        return hi, table - 8.0 * hi

    def arrange(k):
        load(k).wait()
        part = pl.ds(pl.multiple_of(k * LOAD, LOAD), LOAD)
        table = lax.dot_general(
            order, codes_ref[part, :].astype(F32).astype(BF), (((1,), (1,)), ((), ())),
            preferred_element_type=F32,
        )
        hi, lo = split(table[:256])
        hi_ref[0, :, part] = hi
        lo_ref[0, :, part] = lo
        codes_out[:, part] = table[256:]

    loop(0, pieces, arrange)

    partner = (z, q + 1 - 2 * core)

    def send_codes(t):
        piece = pl.ds(pl.multiple_of(t * 32, 32), 32)
        pltpu.make_async_remote_copy(
            codes_out.at[piece], codes_in.at[piece], code_sent, code_came.at[t],
            device_id=partner, device_id_type=MESH,
        ).start()

    pl.semaphore_wait(barrier, Q - 1 + Z - 1)
    pltpu.make_async_remote_copy(
        weight_out, weight_in, weight_sent, weight_came,
        device_id=partner, device_id_type=MESH,
    ).start()
    loop(0, STEPS, send_codes)
    arrived(weight_in, weight_came)
    keep_weights(1, weight_in[:8], weight_in[8:])

    def parts_of(u):
        ends = u >= HALVES - 4
        t = jnp.where(ends, u // 2, 2 * (u // 4) + lax.rem(u, 2))
        return t, jnp.where(ends, lax.rem(u, 2), lax.rem(u // 2, 2))

    def near(t, axis, way):
        on_y = lax.rem(t + axis, 2)
        on_x = 1 - on_y
        nx = lax.rem(x + on_x * way + SIDE, SIDE)
        ny = lax.rem(y + on_y * way + SIDE, SIDE)
        return (z, (ny * SIDE + nx) * 2 + core)

    def spot(t, axis, shift):
        on_y = lax.rem(t + axis, 2)
        here = on_y * y + (1 - on_y) * x
        return lax.rem(here + shift + SIDE, SIDE)

    def block(t, a, b):
        return t * 16 + a * 4 + b

    def send(u, stage, src, dst, device):
        pltpu.make_async_remote_copy(
            src, dst, block_sent, block_came.at[u, stage],
            device_id=device, device_id_type=MESH,
        ).start()

    def a1(u):
        t, h = parts_of(u)
        right, left = near(t, 0, 1), near(t, 0, -1)
        far, r, l = (block(t, spot(t, 0, shift), 2 * h) for shift in (2, 1, -1))
        send(u, 0, hist.at[far], a1_in.at[u, 0], right)
        send(u, 0, hist.at[far + 1], a1_in.at[u, 1], left)
        send(u, 1, hist.at[r + 1], a2_in.at[u, 0, 1], right)
        send(u, 1, hist.at[l], a2_in.at[u, 1, 0], left)

    def a2(u):
        t, h = parts_of(u)
        arrived(a1_in.at[u], block_came.at[u, 0])
        r, l = (block(t, spot(t, 0, shift), 2 * h) for shift in (1, -1))
        hist[r] = hist[r] + a1_in[u, 0]
        hist[l + 1] = hist[l + 1] + a1_in[u, 1]
        send(u, 1, hist.at[r], a2_in.at[u, 0, 0], near(t, 0, 1))
        send(u, 1, hist.at[l + 1], a2_in.at[u, 1, 1], near(t, 0, -1))

    def b1(u):
        t, h = parts_of(u)
        arrived(a2_in.at[u], block_came.at[u, 1])
        first = block(t, spot(t, 0, 0), 2 * h)
        mine = pl.ds(first, 2)
        hist[mine] = hist[mine] + (a2_in[u, 0] + a2_in[u, 1])
        for e in range(2):
            away = lax.rem(2 * h + e - spot(t, 1, 0) + SIDE, SIDE)

            @pl.when(away > 0)
            def _():
                send(u, 2, hist.at[first + e], b_in.at[u, away - 1], near(t, 1, away))

    def plane_sum(u, t):
        arrived(b_in.at[u], block_came.at[u, 2])
        mine = block(t, spot(t, 0, 0), spot(t, 1, 0))
        return mine, (hist[mine] + b_in[u, 0]) + (b_in[u, 1] + b_in[u, 2])

    def to_owner(u):
        t, h = parts_of(u)

        @pl.when((spot(t, 1, 0) // 2 == h) & (t < STEPS - 1))
        def _():
            mine, value = plane_sum(u, t)
            hist[mine] = value
            pltpu.make_async_remote_copy(
                hist.at[mine], z_in.at[t], block_sent, z_came,
                device_id=(lax.rem(z + 1 + t, Z), q), device_id_type=MESH,
            ).start()

    count = iota((16, TILE), 0).astype(F32)
    numbers = [(count + 16.0 * m).astype(BF) for m in range(2)]
    count = (iota((32, TILE), 0) >> 3).astype(F32)
    quads = [(count + 4.0 * m).astype(BF) for m in range(2)]
    passes = 2 * rows // TILE
    span = 1024 // TILE

    def count_group(group):
        counts = None
        for first in range(0, passes, span):
            total = None
            for k in range(first, first + span):
                source, lane = divmod(k * TILE, rows)
                cols = slice(lane, lane + TILE)
                upper, lower = sides(
                    hi_ref, lo_ref, weight_ref[source, :, cols],
                    scale_ref[source, :, cols], source, group * 4, lane, numbers, quads,
                )
                part = lax.dot_general(
                    upper, lower, (((1,), (1,)), ((), ())), preferred_element_type=F32
                )
                total = part if total is None else total + part
            more = classes(total)
            counts = more if counts is None else [a + b for a, b in zip(counts, more)]
        for e in range(2):
            hist[group * 2 + e, 0:32] = counts[2 * e]
            hist[group * 2 + e, 32:64] = counts[2 * e + 1]

    def half_step(u):
        t, h = parts_of(u)

        @pl.when(h == 0)
        def _():
            piece = pl.ds(pl.multiple_of(t * 32, 32), 32)
            arrived(codes_in.at[piece], code_came.at[t])
            hi, lo = split(codes_in[piece])
            hi_ref[1, piece] = hi
            lo_ref[1, piece] = lo

        for a in range(SIDE):
            count_group(t * 8 + 2 * a + h)
        pl.when(u >= LAG_A)(lambda: a2(u - LAG_A))
        a1(u)
        pl.when(u >= LAG_B)(lambda: b1(u - LAG_B))
        pl.when(u >= LAG_Z)(lambda: to_owner(u - LAG_Z))

    loop(0, HALVES, half_step)

    def finish(u):
        pl.when(u < HALVES + LAG_A)(lambda: a2(u - LAG_A))
        pl.when(u < HALVES + LAG_B)(lambda: b1(u - LAG_B))
        pl.when(u < HALVES + LAG_Z)(lambda: to_owner(u - LAG_Z))

    loop(HALVES, HALVES + LAG_Z, finish)
    last = STEPS - 1
    _, summed = plane_sum(HALVES - 2 + spot(last, 1, 0) // 2, last)
    arrived(z_in, z_came)
    summed = summed + jnp.sum(z_in[...], axis=0)
    own_gain[...] = gains(summed, z)

    def send_gain(i):
        pltpu.make_async_remote_copy(
            own_gain, gain_in.at[i - 1], gain_sent, gain_came,
            device_id=(lax.rem(z + i, Z), q), device_id_type=MESH,
        ).start()

    def send_best(i):
        pltpu.make_async_remote_copy(
            own_best, best_in.at[i - 1], best_sent, best_came,
            device_id=(z, lax.rem(q + i, Q)), device_id_type=MESH,
        ).start()

    loop(1, Z, send_gain)
    arrived(gain_in, gain_came)
    together = own_gain[...] + jnp.sum(gain_in[...], axis=0)
    own_best[...] = jnp.broadcast_to(jnp.max(together, axis=1, keepdims=True), (8, 128))
    loop(0, Q - 1, lambda i: send_best(lax.rem(i + 18, Q - 1) + 1))
    for tree in range(2):
        feature_ref[tree] = together[4 * tree : 4 * tree + 4, :16]

    arrived(weight_out, weight_sent)
    arrived(codes_out, code_sent)
    arrived(hist.at[pl.ds(0, STEPS * 16 - 1)], block_sent)
    arrived(gain_in, gain_sent)
    arrived(best_in, best_came)
    best = jnp.maximum(own_best[...], jnp.max(best_in[...], axis=0))
    for tree in range(2):
        chosen = iota((8, 128), 0) == iota((8, 128), 1) + 4 * tree
        line = jnp.sum(jnp.where(chosen, best, 0.0), axis=0, keepdims=True)
        best_ref[tree : tree + 1, :] = line[:, :4]
    arrived(best_in, best_sent)


def hand_over(feature_in, best_in, feature_ref, best_ref):
    feature_ref[...] = feature_in[...]
    best_ref[...] = best_in[...]


def on_device(codes, node_ids, bag_counts, labels):
    rows, features = codes.shape
    dma = pltpu.SemaphoreType.DMA
    whole = pl.BlockSpec(memory_space=pltpu.VMEM)
    outs = [jax.ShapeDtypeStruct((2, 4, 16), F32), jax.ShapeDtypeStruct((2, 4), F32)]
    results = pl.pallas_call(
        kernel,
        out_shape=outs,
        in_specs=[pl.BlockSpec(memory_space=pl.ANY)] * 4,
        out_specs=[whole] * 2,
        scratch_shapes=[
            pltpu.VMEM((rows, features), I32),
            pltpu.VMEM((2, rows), I32),
            pltpu.VMEM((2, rows), I32),
            pltpu.VMEM((1, rows), I32),
            pltpu.VMEM((2, 256, rows), F32),
            pltpu.VMEM((2, 256, rows), F32),
            pltpu.VMEM((256, rows), F32),
            pltpu.VMEM((256, rows), F32),
            pltpu.VMEM((2, 32, rows), F8),
            pltpu.VMEM((2, 16, rows), BF),
            pltpu.VMEM((16, rows), F32),
            pltpu.VMEM((16, rows), F32),
            pltpu.VMEM((STEPS * 16, 64, 128), F32),
            pltpu.VMEM((HALVES, 2, 64, 128), F32),
            pltpu.VMEM((HALVES, 2, 2, 64, 128), F32),
            pltpu.VMEM((HALVES, 3, 64, 128), F32),
            pltpu.VMEM((STEPS - 1, 64, 128), F32),
            pltpu.VMEM((8, 128), F32),
            pltpu.VMEM((Z - 1, 8, 128), F32),
            pltpu.VMEM((8, 128), F32),
            pltpu.VMEM((Q - 1, 8, 128), F32),
            dma((rows // LOAD + 3,)),
            dma(()),
            dma(()),
            dma(()),
            dma(()),
            dma(()),
            dma((STEPS,)),
            dma(()),
            dma((HALVES, 3)),
            dma(()),
            dma(()),
            dma(()),
        ],
        compiler_params=pltpu.CompilerParams(
            collective_id=0, has_side_effects=True, vmem_limit_bytes=60 * 1024 * 1024
        ),
    )(codes, node_ids, bag_counts, labels.reshape(1, rows))
    return pl.pallas_call(
        hand_over, out_shape=outs, in_specs=[whole] * 2, out_specs=[whole] * 2
    )(*results)


def solution(mesh):
    return jax.shard_map(
        on_device,
        mesh=mesh,
        in_specs=(
            P(("rows", "feat"), None),
            P(None, ("rows", "feat")),
            P(None, ("rows", "feat")),
            P(("rows", "feat")),
        ),
        out_specs=(P(None, None, "feat"), P()),
        check_vma=False,
    )
```
